32 devices in a mesh: pod: 1 (over z), dp: 4 (over y), tp: 8 (over x, core).
Axes of the slice: x: 4, y: 4, z: 1, core: 2. Of those that a mesh axis runs over, the one named last changes fastest.
The devices are a block of a 4x4x8 slice.
Arguments:
- x_saved: bfloat16 [6144, 4096], P(('pod', 'dp'))
- h_saved: bfloat16 [6144, 4096], P(('pod', 'dp'))
- mean_one: float32 [6144], P(('pod', 'dp'))
- rstd_one: float32 [6144], P(('pod', 'dp'))
- mean_two: float32 [6144], P(('pod', 'dp'))
- rstd_two: float32 [6144], P(('pod', 'dp'))
- gain_one: bfloat16 [4096], replicated
- gain_two: bfloat16 [4096], replicated
- grad_y: bfloat16 [6144, 4096], P(('pod', 'dp'))
- w_qkv: bfloat16 [4096, 3, 32, 128], P(None, None, 'tp')
- w_proj: bfloat16 [32, 128, 4096], P('tp')
- w_up: bfloat16 [4096, 16384], P(None, 'tp')
- w_down: bfloat16 [16384, 4096], P('tp')
Outputs:
- output 1: bfloat16 [6144, 4096], P(('pod', 'dp'))
- output 2: bfloat16 [4096, 3, 32, 128], P('pod', None, 'tp')
- output 3: bfloat16 [32, 128, 4096], P(('pod', 'tp'))
- output 4: bfloat16 [4096, 16384], P('pod', 'tp')
- output 5: bfloat16 [16384, 4096], P(('pod', 'tp'))
All inputs are finite; a program needn't handle non-finite values.
Results may differ from the reference program's by a relative error of at most 0.0192943.
Values are sent between devices in bfloat16 or wider.
A program may use at most 768 MiB of HBM per device.

```python
import math
import jax
import jax.numpy as jnp
from jax import lax

MODEL_DIM = 4096
NUM_HEADS = 32
FFN_DIM = 16384
TOKENS = 1536
DATA_WAYS = 4

HEAD_DIM = MODEL_DIM // NUM_HEADS
ROW_COUNT = DATA_WAYS * TOKENS
QK_GAIN = (2.0 * math.log(TOKENS)) ** 0.25
GELU_C = math.sqrt(2.0 / math.pi)


def saved_stats(rows_wide):
    row_mean = jnp.mean(rows_wide, axis=-1)
    row_var = jnp.mean(jnp.square(rows_wide - row_mean[:, None]), axis=-1)
    return row_mean, 1.0 / jnp.sqrt(row_var + 1e-5)


def setup_inputs(seed: int = 0, part: int = 0) -> dict:
    shared_keys = jax.random.split(jax.random.key(seed), 6)
    own_keys = jax.random.split(jax.random.fold_in(jax.random.key(seed + 1), part), 7)
    x_rows = jnp.exp(jax.random.uniform(own_keys[3], (ROW_COUNT, 1), jnp.float32, -0.7, 0.7))
    h_rows = jnp.exp(jax.random.uniform(own_keys[4], (ROW_COUNT, 1), jnp.float32, -0.7, 0.7))
    x_shift = 0.5 * jax.random.normal(own_keys[5], (ROW_COUNT, 1), jnp.float32)
    h_shift = 0.5 * jax.random.normal(own_keys[6], (ROW_COUNT, 1), jnp.float32)
    x_saved = (jax.random.normal(own_keys[0], (ROW_COUNT, MODEL_DIM), jnp.float32) * x_rows + x_shift).astype(jnp.bfloat16)
    h_saved = (jax.random.normal(own_keys[1], (ROW_COUNT, MODEL_DIM), jnp.float32) * h_rows + h_shift).astype(jnp.bfloat16)
    grad_y = jax.random.normal(own_keys[2], (ROW_COUNT, MODEL_DIM), jnp.float32).astype(jnp.bfloat16)
    mean_one, rstd_one = saved_stats(x_saved.astype(jnp.float32))
    mean_two, rstd_two = saved_stats(h_saved.astype(jnp.float32))
    gain_one = (1.0 + 0.3 * jax.random.normal(shared_keys[0], (MODEL_DIM,), jnp.float32)).astype(jnp.bfloat16)
    gain_two = (1.0 + 0.3 * jax.random.normal(shared_keys[1], (MODEL_DIM,), jnp.float32)).astype(jnp.bfloat16)
    qkv_scale = jnp.array([QK_GAIN, QK_GAIN, 1.0], jnp.float32)[None, :, None, None] * MODEL_DIM ** -0.5
    w_qkv = (jax.random.normal(shared_keys[2], (MODEL_DIM, 3, NUM_HEADS, HEAD_DIM), jnp.float32) * qkv_scale).astype(jnp.bfloat16)
    w_proj = (jax.random.normal(shared_keys[3], (NUM_HEADS, HEAD_DIM, MODEL_DIM), jnp.float32) * MODEL_DIM ** -0.5).astype(jnp.bfloat16)
    w_up = (jax.random.normal(shared_keys[4], (MODEL_DIM, FFN_DIM), jnp.float32) * MODEL_DIM ** -0.5).astype(jnp.bfloat16)
    w_down = (jax.random.normal(shared_keys[5], (FFN_DIM, MODEL_DIM), jnp.float32) * FFN_DIM ** -0.5).astype(jnp.bfloat16)
    return {'x_saved': x_saved, 'h_saved': h_saved, 'mean_one': mean_one, 'rstd_one': rstd_one,
            'mean_two': mean_two, 'rstd_two': rstd_two, 'gain_one': gain_one, 'gain_two': gain_two,
            'grad_y': grad_y, 'w_qkv': w_qkv, 'w_proj': w_proj, 'w_up': w_up, 'w_down': w_down}


def layer_norm(row_vals, row_mean, row_rstd, gain_vec):
    x_hat = (row_vals.astype(jnp.float32) - row_mean[:, None]) * row_rstd[:, None]
    return x_hat, (x_hat * gain_vec.astype(jnp.float32)).astype(jnp.bfloat16)


def norm_back(d_norm, x_hat, row_rstd, gain_vec):
    scaled = d_norm * gain_vec.astype(jnp.float32)
    scaled_mean = jnp.mean(scaled, axis=-1, keepdims=True)
    proj_mean = jnp.mean(scaled * x_hat, axis=-1, keepdims=True)
    return row_rstd[:, None] * (scaled - scaled_mean - x_hat * proj_mean)


def gelu_pair(pre_act):
    pre_wide = pre_act.astype(jnp.float32)
    tanh_val = jnp.tanh(GELU_C * (pre_wide + 0.044715 * pre_wide * pre_wide * pre_wide))
    gelu_val = 0.5 * pre_wide * (1.0 + tanh_val)
    gelu_slope = 0.5 * (1.0 + tanh_val) + 0.5 * pre_wide * (1.0 - tanh_val * tanh_val) * GELU_C * (1.0 + 0.134145 * pre_wide * pre_wide)
    return gelu_val, gelu_slope


def head_pass(head_in):
    qkv_head, dout_head = head_in
    q_head = qkv_head[:, 0]
    k_head = qkv_head[:, 1]
    v_head = qkv_head[:, 2]
    scores = jnp.dot(q_head, k_head.T, preferred_element_type=jnp.float32) * HEAD_DIM ** -0.5
    row_ids = lax.broadcasted_iota(jnp.int32, (TOKENS, TOKENS), 0)
    col_ids = lax.broadcasted_iota(jnp.int32, (TOKENS, TOKENS), 1)
    scores = jnp.where(col_ids <= row_ids, scores, -1e30)
    shifted = jnp.exp(scores - jnp.max(scores, axis=-1, keepdims=True))
    prob_mat = shifted / jnp.sum(shifted, axis=-1, keepdims=True)
    prob_lo = prob_mat.astype(jnp.bfloat16)
    head_out = jnp.dot(prob_lo, v_head, preferred_element_type=jnp.float32).astype(jnp.bfloat16)
    dv_head = jnp.dot(prob_lo.T, dout_head, preferred_element_type=jnp.float32).astype(jnp.bfloat16)
    d_probs = jnp.dot(dout_head, v_head.T, preferred_element_type=jnp.float32)
    d_scores = (prob_mat * (d_probs - jnp.sum(prob_mat * d_probs, axis=-1, keepdims=True)) * HEAD_DIM ** -0.5).astype(jnp.bfloat16)
    dq_head = jnp.dot(d_scores, k_head, preferred_element_type=jnp.float32).astype(jnp.bfloat16)
    dk_head = jnp.dot(d_scores.T, q_head, preferred_element_type=jnp.float32).astype(jnp.bfloat16)
    return head_out, jnp.stack([dq_head, dk_head, dv_head], axis=1)


def reference(x_saved, h_saved, mean_one, rstd_one, mean_two, rstd_two, gain_one, gain_two, grad_y, w_qkv, w_proj, w_up, w_down):
    qkv_wide = w_qkv.astype(jnp.float32)
    proj_wide = w_proj.astype(jnp.float32)

    def seq_pass(carry, seq_in):
        acc_qkv, acc_proj, acc_up, acc_down = carry
        x_seq, h_seq, mean_a, rstd_a, mean_b, rstd_b, dy_seq = seq_in
        hat_two, norm_two = layer_norm(h_seq, mean_b, rstd_b, gain_two)
        pre_act = jnp.dot(norm_two, w_up, preferred_element_type=jnp.float32).astype(jnp.bfloat16)
        gelu_val, gelu_slope = gelu_pair(pre_act)
        act_out = gelu_val.astype(jnp.bfloat16)
        d_pre = (jnp.dot(dy_seq, w_down.T, preferred_element_type=jnp.float32) * gelu_slope).astype(jnp.bfloat16)
        acc_up = acc_up + jnp.dot(norm_two.T, d_pre, preferred_element_type=jnp.float32)
        acc_down = acc_down + jnp.dot(act_out.T, dy_seq, preferred_element_type=jnp.float32)
        d_norm_two = jnp.dot(d_pre, w_up.T, preferred_element_type=jnp.float32)
        d_mid = dy_seq.astype(jnp.float32) + norm_back(d_norm_two, hat_two, rstd_b, gain_two)
        d_mid_lo = d_mid.astype(jnp.bfloat16)
        hat_one, norm_one = layer_norm(x_seq, mean_a, rstd_a, gain_one)
        qkv_heads = jnp.einsum('td,dche->tche', norm_one.astype(jnp.float32), qkv_wide).astype(jnp.bfloat16)
        d_attn = jnp.einsum('td,hed->the', d_mid_lo.astype(jnp.float32), proj_wide).astype(jnp.bfloat16)
        head_outs, head_grads = lax.map(head_pass, (jnp.moveaxis(qkv_heads, 2, 0), jnp.moveaxis(d_attn, 1, 0)))
        attn_out = jnp.moveaxis(head_outs, 0, 1)
        d_qkv = jnp.moveaxis(head_grads, 0, 2).astype(jnp.float32)
        acc_proj = acc_proj + jnp.einsum('the,td->hed', attn_out.astype(jnp.float32), d_mid_lo.astype(jnp.float32))
        acc_qkv = acc_qkv + jnp.einsum('td,tche->dche', norm_one.astype(jnp.float32), d_qkv)
        d_norm_one = jnp.einsum('tche,dche->td', d_qkv, qkv_wide)
        grad_x = (d_mid + norm_back(d_norm_one, hat_one, rstd_a, gain_one)).astype(jnp.bfloat16)
        return (acc_qkv, acc_proj, acc_up, acc_down), grad_x

    zero_sums = (jnp.zeros((MODEL_DIM, 3, NUM_HEADS, HEAD_DIM), jnp.float32),
                 jnp.zeros((NUM_HEADS, HEAD_DIM, MODEL_DIM), jnp.float32),
                 jnp.zeros((MODEL_DIM, FFN_DIM), jnp.float32),
                 jnp.zeros((FFN_DIM, MODEL_DIM), jnp.float32))
    seq_inputs = (x_saved.reshape(DATA_WAYS, TOKENS, MODEL_DIM), h_saved.reshape(DATA_WAYS, TOKENS, MODEL_DIM),
                  mean_one.reshape(DATA_WAYS, TOKENS), rstd_one.reshape(DATA_WAYS, TOKENS),
                  mean_two.reshape(DATA_WAYS, TOKENS), rstd_two.reshape(DATA_WAYS, TOKENS),
                  grad_y.reshape(DATA_WAYS, TOKENS, MODEL_DIM))
    grad_sums, grad_rows = lax.scan(seq_pass, zero_sums, seq_inputs)
    acc_qkv, acc_proj, acc_up, acc_down = grad_sums
    return (grad_rows.reshape(ROW_COUNT, MODEL_DIM), acc_qkv.astype(jnp.bfloat16), acc_proj.astype(jnp.bfloat16),
            acc_up.astype(jnp.bfloat16), acc_down.astype(jnp.bfloat16))
```

```python
import functools
import math
import jax
import jax.numpy as jnp
from jax import lax
from jax.experimental import pallas as pl
from jax.experimental.pallas import tpu as pltpu
from jax.sharding import PartitionSpec as P

GELU_C = math.sqrt(2.0 / math.pi)
VMEM_BYTES = 60 * 1024 * 1024
F32 = jnp.float32
BF16 = jnp.bfloat16


def layer_norm(row_vals, row_mean, row_rstd, gain_vec):
    x_hat = (row_vals.astype(F32) - row_mean[:, None]) * row_rstd[:, None]
    return x_hat, (x_hat * gain_vec.astype(F32)).astype(BF16)


def norm_back(d_norm, x_hat, row_rstd, gain_vec):
    scaled = d_norm * gain_vec.astype(F32)
    scaled_mean = jnp.mean(scaled, axis=-1, keepdims=True)
    proj_mean = jnp.mean(scaled * x_hat, axis=-1, keepdims=True)
    return row_rstd[:, None] * (scaled - scaled_mean - x_hat * proj_mean)


def gelu_pair(pre_wide):
    square = pre_wide * pre_wide
    half_up = 0.5 + 0.5 * jnp.tanh(pre_wide * (GELU_C + (GELU_C * 0.044715) * square))
    gelu_val = pre_wide * half_up
    gelu_slope = half_up + gelu_val * (1.0 - half_up) * (2.0 * GELU_C + (2.0 * GELU_C * 0.134145) * square)
    return gelu_val, gelu_slope


def hold(*values):
    return lax.optimization_barrier(values)


def tile_of(size, want):
    return want if size % want == 0 else size


def up_proj(first_block, norm_rows, w_up, row_count, row_tile):
    total, depth = norm_rows.shape
    cols = w_up.shape[1]
    col_tile = tile_of(cols, 1024)
    blocks = total // row_tile

    def body(first, n_ref, w_ref, out_ref):
        out_ref[...] = jnp.dot(n_ref[...], w_ref[...], preferred_element_type=F32).astype(BF16)

    return pl.pallas_call(
        body,
        out_shape=jax.ShapeDtypeStruct((row_count, cols), BF16),
        grid_spec=pltpu.PrefetchScalarGridSpec(
            num_scalar_prefetch=1, grid=(row_count // row_tile, cols // col_tile),
            in_specs=[pl.BlockSpec((row_tile, depth), lambda i, j, first: (lax.rem(first[0] + i, blocks), 0)),
                      pl.BlockSpec((depth, col_tile), lambda i, j, first: (0, j))],
            out_specs=pl.BlockSpec((row_tile, col_tile), lambda i, j, first: (i, j))),
        compiler_params=pltpu.CompilerParams(vmem_limit_bytes=VMEM_BYTES),
        cost_estimate=pl.CostEstimate(flops=2 * row_count * depth * cols, transcendentals=0,
                                      bytes_accessed=2 * (row_count * (depth + cols) + depth * cols)),
        name="up_proj",
    )(first_block, norm_rows, w_up)


def down_back(first_block, grad_rows, w_down, pre_act, row_tile, total, prior=None):
    row_count, cols = pre_act.shape
    depth = grad_rows.shape[1]
    col_tile = tile_of(cols, 512)
    out_blocks = total // row_tile
    local = prior is None

    def body(first, d_ref, w_ref, a_ref, *rest):
        outs = rest if local else rest[2:]
        sub = tile_of(col_tile, 256)
        for at in range(0, col_tile, sub):
            d_act = lax.dot_general(d_ref[...], w_ref[at:at + sub, :], (((1,), (1,)), ((), ())), preferred_element_type=F32)
            gelu_val, gelu_slope = gelu_pair(a_ref[:, at:at + sub].astype(F32))
            d_pre = (d_act * gelu_slope).astype(BF16)
            outs[0][:, at:at + sub] = gelu_val.astype(BF16)
            outs[1][:, at:at + sub] = d_pre
            if local:
                outs[2][:, at:at + sub] = d_pre

    wrap = lambda i, j, first: (lax.rem(first[0] + i, out_blocks), j)
    in_rows = (lambda i, j, first: (i, 0)) if local else (lambda i, j, first: (lax.rem(first[0] + i, out_blocks), 0))
    in_specs = [pl.BlockSpec((row_tile, depth), in_rows),
                pl.BlockSpec((col_tile, depth), lambda i, j, first: (j, 0)),
                pl.BlockSpec((row_tile, col_tile), lambda i, j, first: (i, j))]
    out_specs = [pl.BlockSpec((row_tile, col_tile), wrap)] * 2
    out_shape = [jax.ShapeDtypeStruct((total, cols), BF16)] * 2
    args = [first_block, grad_rows, w_down, pre_act]
    aliases = {}
    if local:
        out_specs = out_specs + [pl.BlockSpec((row_tile, col_tile), lambda i, j, first: (i, j))]
        out_shape = out_shape + [jax.ShapeDtypeStruct((row_count, cols), BF16)]
    else:
        in_specs = in_specs + [pl.BlockSpec(memory_space=pl.ANY)] * 2
        args = args + list(prior)
        aliases = {4: 0, 5: 1}
    return pl.pallas_call(
        body,
        out_shape=out_shape,
        grid_spec=pltpu.PrefetchScalarGridSpec(
            num_scalar_prefetch=1, grid=(row_count // row_tile, cols // col_tile),
            in_specs=in_specs, out_specs=out_specs),
        input_output_aliases=aliases,
        compiler_params=pltpu.CompilerParams(vmem_limit_bytes=VMEM_BYTES),
        cost_estimate=pl.CostEstimate(flops=2 * row_count * depth * cols, transcendentals=row_count * cols,
                                      bytes_accessed=2 * (row_count * (depth + 3 * cols) + depth * cols)),
        name="down_back",
    )(*args)


def attention_back(qkv, d_attn):
    _, heads, toks, size = qkv.shape
    q_tile = tile_of(toks, 512)
    steps = toks // q_tile
    scale = size ** -0.5

    def dot(a, b, ca, cb):
        return lax.dot_general(a, b, (((ca,), (cb,)), ((), ())), preferred_element_type=F32)

    def body(q_ref, k_ref, v_ref, do_ref, o_ref, g_ref, dk_acc, dv_acc):
        step = pl.program_id(1)

        @pl.when(step == 0)
        def _():
            dk_acc[...] = jnp.zeros_like(dk_acc)
            dv_acc[...] = jnp.zeros_like(dv_acc)

        def block(n):
            seen = (n + 1) * q_tile
            q, d_out = q_ref[0, 0], do_ref[0]
            k, v = k_ref[0, 0, :seen, :], v_ref[0, 0, :seen, :]
            scores = dot(q, k, 1, 1) * scale
            rows = lax.broadcasted_iota(jnp.int32, (q_tile, seen), 0) + n * q_tile
            cols = lax.broadcasted_iota(jnp.int32, (q_tile, seen), 1)
            scores = jnp.where(cols <= rows, scores, -1e30)
            shifted = jnp.exp(scores - jnp.max(scores, axis=-1, keepdims=True))
            probs = shifted * (1.0 / jnp.sum(shifted, axis=-1, keepdims=True))
            probs_lo = probs.astype(BF16)
            o_ref[0] = dot(probs_lo, v, 1, 0).astype(BF16)
            dv_acc[:seen, :] += dot(probs_lo, d_out, 0, 0)
            d_probs = dot(d_out, v, 1, 1)
            inner = jnp.sum(probs * d_probs, axis=-1, keepdims=True)
            d_scores = (probs * (d_probs - inner) * scale).astype(BF16)
            g_ref[0, 0, n * q_tile:seen, :] = dot(d_scores, k, 1, 0).astype(BF16)
            dk_acc[:seen, :] += dot(d_scores, q, 0, 0)

        for n in range(steps):
            pl.when(step == n)(functools.partial(block, n))

        @pl.when(step == steps - 1)
        def _():
            g_ref[1, 0] = dk_acc[...].astype(BF16)
            g_ref[2, 0] = dv_acc[...].astype(BF16)

    return pl.pallas_call(
        body,
        out_shape=[jax.ShapeDtypeStruct((heads, toks, size), BF16), jax.ShapeDtypeStruct(qkv.shape, BF16)],
        grid=(heads, steps),
        in_specs=[pl.BlockSpec((1, 1, q_tile, size), lambda h, i: (0, h, i, 0)),
                  pl.BlockSpec((1, 1, toks, size), lambda h, i: (1, h, 0, 0)),
                  pl.BlockSpec((1, 1, toks, size), lambda h, i: (2, h, 0, 0)),
                  pl.BlockSpec((1, q_tile, size), lambda h, i: (h, i, 0))],
        out_specs=[pl.BlockSpec((1, q_tile, size), lambda h, i: (h, i, 0)),
                   pl.BlockSpec((3, 1, toks, size), lambda h, i: (0, h, 0, 0))],
        scratch_shapes=[pltpu.VMEM((toks, size), F32), pltpu.VMEM((toks, size), F32)],
        compiler_params=pltpu.CompilerParams(vmem_limit_bytes=VMEM_BYTES),
        cost_estimate=pl.CostEstimate(flops=40 * heads * toks * toks * size, transcendentals=heads * toks * toks,
                                      bytes_accessed=2 * 8 * heads * toks * size),
        name="attention_back",
    )(qkv, qkv, qkv, d_attn)


def solution(mesh):
    row_spec = P(('pod', 'dp'), None)
    stat_spec = P(('pod', 'dp'))
    in_specs = (row_spec, row_spec, stat_spec, stat_spec, stat_spec, stat_spec, P(None), P(None), row_spec,
                P(None, None, 'tp', None), P('tp', None, None), P(None, 'tp'), P('tp', None))
    out_specs = (row_spec, P('pod', None, 'tp', None), P(('pod', 'tp'), None, None), P('pod', 'tp'), P(('pod', 'tp'), None))
    tp_ways, dp_ways = mesh.shape['tp'], mesh.shape['dp']

    def layer_step(x_saved, h_saved, mean_one, rstd_one, mean_two, rstd_two, gain_one, gain_two, grad_y, w_qkv, w_proj, w_up, w_down):
        toks, width = x_saved.shape
        share = toks // tp_ways
        total = toks * dp_ways
        tp_at, dp_at = lax.axis_index('tp'), lax.axis_index('dp')
        mine = lambda a: lax.dynamic_slice_in_dim(a, tp_at * share, share, 0)
        row_tile = tile_of(toks, 512)
        seq_blocks = toks // row_tile
        later = lambda n: ((dp_at + n) * seq_blocks).astype(jnp.int32).reshape(1)
        zero_block = jnp.zeros((1,), jnp.int32)

        dy_mine = mine(grad_y)
        hat_two, norm_two_mine = layer_norm(mine(h_saved), mine(mean_two), mine(rstd_two), gain_two)
        norm_two_all = lax.all_gather(norm_two_mine, ('dp', 'tp'), tiled=True)

        _, norm_two = layer_norm(h_saved, mean_two, rstd_two, gain_two)
        pre_own = up_proj(zero_block, norm_two, w_up, toks, row_tile)
        act_all, d_pre_all, d_pre_own = down_back(later(0), grad_y, w_down, pre_own, row_tile, total)
        part_two = lax.dot_general(d_pre_own, w_up, (((1,), (1,)), ((), ())), preferred_element_type=F32).astype(BF16)
        d_norm_two = lax.psum_scatter(part_two, 'tp', scatter_dimension=0, tiled=True)

        _, norm_one = layer_norm(x_saved, mean_one, rstd_one, gain_one)
        qkv = jnp.einsum('td,dche->chte', norm_one, w_qkv, preferred_element_type=F32).astype(BF16)
        norm_two_all, qkv = hold(norm_two_all, qkv)
        pre_next = up_proj(later(1), norm_two_all, w_up, toks, row_tile)

        d_norm_two, pre_next, dy_mine = hold(d_norm_two, pre_next, dy_mine)
        d_mid = dy_mine.astype(F32) + norm_back(d_norm_two.astype(F32), hat_two, mine(rstd_two), gain_two)
        d_mid_mine, norm_two_all, dy_mine = hold(d_mid.astype(BF16), norm_two_all, dy_mine)
        d_mid_lo = lax.all_gather(d_mid_mine, 'tp', tiled=True)
        dy_all = lax.all_gather(dy_mine, ('dp', 'tp'), tiled=True)
        pre_rest = up_proj(later(2), norm_two_all, w_up, total - 2 * toks, row_tile)

        d_mid_lo, pre_rest = hold(d_mid_lo, pre_rest)
        d_attn = jnp.einsum('td,hed->hte', d_mid_lo, w_proj, preferred_element_type=F32).astype(BF16)
        attn_out, d_qkv = attention_back(qkv, d_attn)

        sum_proj = jnp.einsum('hte,td->hed', attn_out, d_mid_lo, preferred_element_type=F32).reshape(-1, width)
        sum_qkv = jnp.einsum('chte,td->ched', d_qkv, norm_one, preferred_element_type=F32).reshape(-1, width)
        sum_proj = lax.psum_scatter(sum_proj, 'dp', scatter_dimension=0, tiled=True)
        sum_qkv = lax.psum_scatter(sum_qkv, 'dp', scatter_dimension=0, tiled=True)

        part_one = jnp.einsum('chte,dche->td', d_qkv, w_qkv, preferred_element_type=F32).astype(BF16)
        parts_one = lax.all_to_all(part_one.reshape(tp_ways, share, width), 'tp', 0, 0)

        act_all, d_pre_all = down_back(later(1), dy_all, w_down, pre_next, row_tile, total, (act_all, d_pre_all))
        d_pre_all, parts_one = hold(d_pre_all, parts_one)
        d_norm_one = jnp.sum(parts_one.astype(F32), axis=0)
        hat_one, _ = layer_norm(mine(x_saved), mine(mean_one), mine(rstd_one), gain_one)
        grad_x_mine = (d_mid + norm_back(d_norm_one, hat_one, mine(rstd_one), gain_one)).astype(BF16)
        pre_rest, grad_x_mine = hold(pre_rest, grad_x_mine)
        moved = [lax.ppermute(grad_x_mine, 'tp', [(i, (i + n) % tp_ways) for i in range(tp_ways)]) for n in range(1, tp_ways)]
        act_all, d_pre_all = down_back(later(2), dy_all, w_down, pre_rest, row_tile, total, (act_all, d_pre_all))
        d_pre_all, sum_proj = hold(d_pre_all, sum_proj)
        proj_piece = sum_proj.astype(BF16)
        act_all, proj_piece = hold(act_all, proj_piece)
        grad_proj = lax.all_gather(proj_piece, 'dp', tiled=True).reshape(w_proj.shape)
        grad_down = lax.dot_general(act_all, dy_all, (((0,), (0,)), ((), ())), preferred_element_type=F32).astype(BF16)

        grad_down, sum_qkv, *moved = hold(grad_down, sum_qkv, *moved)
        grad_x = jnp.zeros(x_saved.shape, BF16)
        for n, rows in enumerate([grad_x_mine] + moved):
            grad_x = lax.dynamic_update_slice_in_dim(grad_x, rows, lax.rem(tp_at + tp_ways - n, tp_ways) * share, 0)
        qkv_piece = jnp.swapaxes(sum_qkv.astype(BF16).reshape(-1, qkv.shape[3], width), 1, 2).reshape(-1, qkv.shape[3])
        norm_two_all, qkv_piece = hold(norm_two_all, qkv_piece)
        grad_qkv = lax.all_gather(qkv_piece, 'dp', tiled=True)
        grad_qkv = jnp.moveaxis(grad_qkv.reshape(qkv.shape[:2] + (width, qkv.shape[3])), 2, 0)
        grad_up = lax.dot_general(norm_two_all, d_pre_all, (((0,), (0,)), ((), ())), preferred_element_type=F32).astype(BF16)
        return grad_x, grad_qkv, grad_proj, grad_up, grad_down

    return jax.shard_map(layer_step, mesh=mesh, in_specs=in_specs, out_specs=out_specs, check_vma=False)
```
